256 devices in a mesh: tm: 64 (over z, y, x_hi), pair: 4 (over x_lo, core).
Axes of the slice: x: 4 (x_hi: 2, x_lo: 2; x = x_hi * 2 + x_lo), y: 4, z: 8, core: 2. Of those that a mesh axis runs over, the one named last changes fastest.
Arguments:
- x_path: bfloat16 [8, 32768, 512], P('pair', 'tm'), parts along dimension 0, may hold values from -0.19921875 to 0.19921875
- x_anchor: bfloat16 [8, 512], P('pair'), parts along dimension 0, may hold values from -0.19921875 to 0.19921875
- y_steps: bfloat16 [8, 8192, 512], P('pair', 'tm'), parts along dimension 0, may hold values from -0.14941406 to 0.14941406
- left_in: float32 [16, 32768], P('pair', 'tm'), parts along dimension 0, may hold values from 0.5 to 1.5
- bottom_in: float32 [16, 8192], P('pair', 'tm'), parts along dimension 0, may hold values from 0.5 to 1.5
- corner_in: float32 [16, 64], P('pair', 'tm'), parts along dimension 0, may hold values from 0.5 to 1.5
Outputs:
- right_out: float32 [16, 32768], P('pair', 'tm'), parts along dimension 0
- top_out: float32 [16, 49152], P('pair', 'tm'), parts along dimension 0
The draws below stay inside these ranges and needn't reach their ends.
There are 4 independent parts, one for each index of `pair`. The reference program is written for one: setup_inputs(seed, part) draws one part's arguments, and reference() takes and returns one part's arrays. A program takes and returns all parts, laid end to end along the dimension named above; each array names one. Nothing has to cross between parts.
All inputs are finite; a program needn't handle non-finite values.
Results may differ from the reference program's by a relative error of at most 0.00094.
Values may be sent and summed in bfloat16 or wider, within the bound.
A program may use at most 64 MiB of HBM per device.

```python
import jax
import jax.numpy as jnp
from jax import lax

CH = 512
TILE = 128
TX = 512
SX = 2
SY = 2
TICKS = 6
PASSES = 4
PAIRS = 4
XLEN = 32768
YLEN = 8192
N_TM = 64


def steps_of(key, dims, shards, low, largest):
    loudness = 1.0
    for position, parts in shards:
        draws = jax.random.uniform(jax.random.fold_in(jax.random.fold_in(key, 6), position), (parts,), jnp.float32, low / len(shards), largest / len(shards))
        loudness = loudness * jnp.repeat(jnp.exp(draws), dims[position] // parts).reshape((-1,) + (1,) * (len(dims) - 1 - position))
    return loudness


def bell_draw(stream_key, extent, deviation, bound, split=(), kind=jnp.bfloat16):
    loudness = steps_of(stream_key, extent, split, -0.22, 0.18) if split else 1.0
    array = jax.random.normal(stream_key, extent, jnp.float32) * deviation * loudness
    return jnp.minimum(jnp.maximum(array, -bound), bound).astype(kind)


def setup_inputs(seed: int = 0, part: int = 0) -> dict:
    seeds = jax.random.split(jax.random.key(seed), 7)
    part_keys = jax.random.split(jax.random.fold_in(seeds[6], part), 7)
    x_path = bell_draw(part_keys[0], (SX, XLEN, CH), 0.03, 0.19921875, ((1, 64),))
    x_anchor = bell_draw(part_keys[1], (SX, CH), 0.03, 0.19921875)
    y_steps = bell_draw(part_keys[2], (SY, YLEN, CH), 0.02, 0.14941406, ((1, 64),))
    left_in = jnp.clip(0.5 + 1.0 * jax.random.uniform(part_keys[3], (PAIRS, XLEN), jnp.float32) ** steps_of(part_keys[3], (PAIRS, XLEN), ((1, 64),), -0.2, 0.2), 0.5, 1.5)
    bottom_in = jnp.clip(0.5 + 1.0 * jax.random.uniform(part_keys[4], (PAIRS, YLEN), jnp.float32) ** steps_of(part_keys[4], (PAIRS, YLEN), ((1, 64),), -0.2, 0.2), 0.5, 1.5)
    corner_in = jnp.clip(0.5 + 1.0 * jax.random.uniform(part_keys[5], (PAIRS, N_TM), jnp.float32) ** steps_of(part_keys[5], (PAIRS, N_TM), ((1, 64),), -0.2, 0.2), 0.5, 1.5)
    return {"x_path": x_path, "x_anchor": x_anchor, "y_steps": y_steps, "left_in": left_in, "bottom_in": bottom_in, "corner_in": corner_in}


def picard(left_edge, bottom, corner, products, lower_ones):
    initial = left_edge[..., :, None] + bottom[..., None, :] - corner[..., None, None]
    kernel_grid = initial
    lower_row = jnp.concatenate([corner[..., None], bottom[..., :-1]], axis=-1)[..., None, :]
    for sweep in range(PASSES):
        inner_rows = jnp.concatenate([left_edge[..., :-1, None], kernel_grid[..., :-1, :-1]], axis=-1)
        node_values = jnp.concatenate([lower_row, inner_rows], axis=-2)
        partial_value = jnp.einsum("ab,...bc->...ac", lower_ones, node_values * products, precision=lax.Precision.HIGHEST)
        kernel_grid = initial + jnp.einsum("...ac,dc->...ad", partial_value, lower_ones, precision=lax.Precision.HIGHEST)
    return kernel_grid


def reference(x_path, x_anchor, y_steps, left_in, bottom_in, corner_in):
    count_tm = N_TM
    earlier = jnp.concatenate([x_anchor[:, None, :], x_path[:, :-1, :]], axis=1)
    steps_x = (x_path.astype(jnp.float32) - earlier.astype(jnp.float32)).astype(jnp.bfloat16)
    x_blocks = steps_x.reshape(SX, count_tm, TX, CH).astype(jnp.float32)
    y_blocks = y_steps.reshape(SY, count_tm, TILE, CH)
    positions = jnp.arange(TILE)
    lower_ones = (positions[:, None] >= positions[None, :]).astype(jnp.float32)
    row_count = TX // TILE
    left_edges = left_in.reshape(PAIRS, count_tm, TX).transpose(1, 0, 2)
    bottom = bottom_in.reshape(PAIRS, count_tm, TILE).transpose(1, 0, 2)
    corner = corner_in.transpose(1, 0)
    bottom_row = jnp.arange(count_tm)[:, None] == 0
    bottom = jnp.where(bottom_row[:, :, None], jnp.float32(1.0), bottom)
    corner = jnp.where(bottom_row, jnp.float32(1.0), corner)
    top_edges = []
    top_edge = bottom
    for tick_index in range(TICKS):
        if tick_index > 0:
            corner = bottom[..., -1]
            bottom = jnp.concatenate([jnp.ones((1, PAIRS, TILE), jnp.float32), top_edge[:-1]], axis=0)
        y_now = jnp.roll(y_blocks, tick_index, axis=1).astype(jnp.float32)
        products = jnp.einsum("xisc,yitc->ixyst", x_blocks, y_now, precision=lax.Precision.HIGHEST)
        products = products.reshape(count_tm, PAIRS, TX, TILE)
        bottom_now = bottom
        corner_now = corner
        rights = []
        for level in range(row_count):
            left_edge = left_edges[..., level * TILE:(level + 1) * TILE]
            kernel_grid = picard(left_edge, bottom_now, corner_now, products[:, :, level * TILE:(level + 1) * TILE, :], lower_ones)
            rights.append(kernel_grid[..., :, -1])
            corner_now = left_edge[..., -1]
            bottom_now = kernel_grid[..., -1, :]
        top_edge = bottom_now
        top_edges.append(top_edge)
        left_edges = jnp.concatenate(rights, axis=-1)
    right_out = left_edges.transpose(1, 0, 2).reshape(PAIRS, count_tm * TX)
    top_out = jnp.stack(top_edges, axis=2).transpose(1, 0, 2, 3).reshape(PAIRS, count_tm * TICKS * TILE)
    return right_out, top_out
```

```python
import functools

import jax
import jax.numpy as jnp
from jax import lax
from jax.experimental import pallas as pl
from jax.experimental.pallas import tpu as pltpu
from jax.sharding import PartitionSpec as P

MESH = pl.DeviceIdType.MESH
TICKS = 6
HOPS = TICKS - 1
TILE = 128
LEVELS = 4
PAIRS = 4
GROUPS = TILE // 8
F32 = jnp.float32
BF16 = jnp.bfloat16


def iota(shape, axis):
    return lax.broadcasted_iota(jnp.int32, shape, axis)


def tile_row(shape):
    place = iota(shape, 0)
    return (place % 8) * GROUPS + place // 8


def split_dot(rows, weights):
    high = rows.astype(BF16)
    low = (rows - high.astype(F32)).astype(BF16)
    return jnp.dot(jnp.concatenate([high, low], axis=1), weights, preferred_element_type=F32)


def vectors(tile):
    return [tile[8 * j : 8 * j + 8] for j in range(GROUPS)]


def stacked(parts):
    return jnp.concatenate(parts, axis=0)


def before_rows(tile):
    sub = iota((8, TILE), 0)
    running = jnp.zeros((8, TILE), F32)
    sums = []
    for part in vectors(tile):
        sums.append(running)
        running = running + part
    scan = running
    for step in (1, 2, 4):
        scan = scan + jnp.where(sub >= step, pltpu.roll(scan, step, axis=0), 0.0)
    offset = scan - running
    return stacked([s + offset for s in sums])


def all_rows(tile):
    parts = vectors(tile)
    while len(parts) > 1:
        parts = [a + b for a, b in zip(parts[::2], parts[1::2])]
    total = parts[0]
    for step in (4, 2, 1):
        total = total + pltpu.roll(total, step, axis=0)
    return total


def repeated(row):
    return stacked([row] * GROUPS)


def rows_of_pairs(values):
    sub = iota((8, TILE), 0)
    out = values[-1]
    for k in range(len(values) - 2, -1, -1):
        out = jnp.where(sub == k, values[k], out)
    return out


def kernel(
    x_ref, anchor_ref, y_ref, left_ref, bottom_ref, corner_ref, right_ref, top_ref,
    steps, prod, minus, plus, lead, lam, last, edge, corner, tri, ones,
    xs, xgot, ybuf, note, heard,
    xs_send, xs_recv, y_send, y_recv, note_send, note_recv,
):
    count = lax.axis_size("tm")
    me, part = lax.axis_index("tm"), lax.axis_index("pair")
    at_start = me == 0
    next1, next2 = lax.rem(me + 1, count), lax.rem(me + 2, count)
    prev1, prev2 = lax.rem(me + count - 1, count), lax.rem(me + count - 2, count)

    barrier = pltpu.get_barrier_semaphore()
    for other in (prev1, prev2):
        pl.semaphore_signal(barrier, inc=1, device_id=(other, part), device_id_type=MESH)

    for m in range(2):
        tail = x_ref[m, 496:512, :].astype(F32)[15:16]
        for c in range(4):
            xs[m * 4 + c : m * 4 + c + 1, :] = tail[:, c * 128 : (c + 1) * 128]

    def x_copy():
        return pltpu.make_async_remote_copy(
            src_ref=xs, dst_ref=xgot, send_sem=xs_send, recv_sem=xs_recv,
            device_id=(next1, part), device_id_type=MESH,
        )

    def y_copy(source, slot, sem, to):
        return pltpu.make_async_remote_copy(
            src_ref=source, dst_ref=ybuf.at[slot], send_sem=y_send.at[sem], recv_sem=y_recv.at[slot],
            device_id=(to, part), device_id_type=MESH,
        )

    def note_copy(t):
        return pltpu.make_async_remote_copy(
            src_ref=note.at[t], dst_ref=heard.at[t], send_sem=note_send.at[t], recv_sem=note_recv.at[t],
            device_id=(next1, part), device_id_type=MESH,
        )

    pl.semaphore_wait(barrier, 2)
    x_copy().start()
    y_copy(y_ref, 0, 0, next1).start()
    y_copy(y_ref, 1, 1, next2).start()

    from_row = iota((2 * TILE, TILE), 0) % TILE
    tri[...] = jnp.where(from_row < iota((2 * TILE, TILE), 1), 1.0, 0.0).astype(BF16)
    ones[...] = jnp.ones((2 * TILE, TILE), BF16)
    row_here, lane = tile_row((TILE, TILE)), iota((TILE, TILE), 1)
    differ = jnp.where(lane == row_here, 1.0, jnp.where(lane == row_here - 1, -1.0, 0.0)).astype(BF16)
    lane_row = iota((8, TILE), 1)

    for p in range(PAIRS):
        start = jnp.broadcast_to(corner_ref[p : p + 1, 0:1], (8, TILE))
        start = jnp.where(at_start, 1.0, start)
        corner[0, p] = start
        for r in range(LEVELS):
            at = (r + 1) * TILE - 1
            corner[r + 1, p] = jnp.broadcast_to(left_ref[p : p + 1, at : at + 1], (8, TILE))
        bottom = jnp.broadcast_to(bottom_ref[p : p + 1, :], (8, TILE))
        shifted = jnp.where(lane_row == 0, start, pltpu.roll(bottom, 1, axis=1))
        edge[0, p] = jnp.where(at_start, 0.0, bottom - shifted)
    for r in range(LEVELS):
        picked = []
        for p in range(PAIRS):
            row = jnp.broadcast_to(left_ref[p : p + 1, r * TILE : (r + 1) * TILE], (8, TILE)) - corner[r, p]
            picked.append(jnp.where(lane == row_here - 1, repeated(row), 0.0))
        spread = split_dot(stacked(picked), ones[...])
        for p in range(PAIRS):
            lam[r, p] = spread[p * TILE : (p + 1) * TILE]

    def increments(m, r, previous):
        found = jnp.dot(differ, x_ref[m, r * TILE : (r + 1) * TILE, :], preferred_element_type=F32)
        found = jnp.where(iota((TILE, 512), 0) == 0, found - previous, found)
        steps[m, r * TILE : (r + 1) * TILE, :] = found.astype(BF16)

    for m in range(2):
        for r in range(1, LEVELS):
            increments(m, r, x_ref[m, r * TILE - 16 : r * TILE, :].astype(F32)[15:16])
    x_copy().wait_recv()
    for m in range(2):
        came = jnp.concatenate([xgot[m * 4 + c : m * 4 + c + 1, :] for c in range(4)], axis=1)
        increments(m, 0, jnp.where(at_start, anchor_ref[m : m + 1, :].astype(F32), came))

    def prepare(y_of):
        for m in range(2):
            for n in range(2):
                found = lax.dot_general(
                    steps[m], y_of(n), (((1,), (1,)), ((), ())), preferred_element_type=F32
                )
                for r in range(LEVELS):
                    prod[r, 2 * m + n] = found[r * TILE : (r + 1) * TILE]

        def level(r, carry):
            across = split_dot(stacked([prod[r, p] for p in range(PAIRS)]), tri[...])
            for p in range(PAIRS):
                wide = across[p * TILE : (p + 1) * TILE]
                both = before_rows(wide)
                down = before_rows(prod[r, p])
                minus[r, p] = -(both + down)
                plus[r, p] = 1.0 + both
                edge_part = lam[r, p]
                lead[r, p] = edge_part + before_rows(edge_part * wide)
            return carry

        lax.fori_loop(0, LEVELS, level, 0)

    def chain():
        def level(r, carry):
            bottoms = [edge[r, p] for p in range(PAIRS)]
            rows = [repeated(bottoms[p]) * minus[r, p] for p in range(PAIRS)]
            grids, bases = [None] * PAIRS, [None] * PAIRS
            for a, b in ((0, 1), (2, 3)):
                out = split_dot(stacked([rows[a], rows[b], bottoms[a], bottoms[b]]), tri[...])
                for k, p in enumerate((a, b)):
                    low = corner[r, p] + out[2 * TILE + 8 * k : 2 * TILE + 8 * k + 8]
                    low = repeated(low)
                    bases[p] = lam[r, p] + low
                    grids[p] = lead[r, p] + low * plus[r, p] + out[k * TILE : (k + 1) * TILE]
            for sweep in range(2):
                for a, b in ((0, 1), (2, 3)):
                    out = split_dot(
                        stacked([before_rows(prod[r, a] * grids[a]), before_rows(prod[r, b] * grids[b])]), tri[...]
                    )
                    for k, p in enumerate((a, b)):
                        grids[p] = bases[p] + out[k * TILE : (k + 1) * TILE]
            for p in range(PAIRS):
                final = prod[r, p] * grids[p]
                last[r, p] = final
                edge[r + 1, p] = bottoms[p] + all_rows(final)
            return carry

        lax.fori_loop(0, LEVELS, level, 0)

    def send_note(t):
        note[t] = rows_of_pairs([edge[LEVELS, p] for p in range(PAIRS)] + [corner[LEVELS, p] for p in range(PAIRS)])
        note_copy(t).start()

    def settle(t):
        tops = [edge[LEVELS, p] for p in range(PAIRS)]
        out = split_dot(stacked(tops), tri[...])
        whole = rows_of_pairs([corner[LEVELS, p] + tops[p] + out[8 * p : 8 * p + 8] for p in range(PAIRS)])
        top_ref[:, pl.ds(pl.multiple_of(t * TILE, TILE), TILE)] = whole[:PAIRS]

        def level(r, carry):
            out = split_dot(stacked([before_rows(last[r, p]) for p in range(PAIRS)]), ones[...])
            for p in range(PAIRS):
                lam[r, p] = lam[r, p] + out[p * TILE : (p + 1) * TILE]
            return carry

        lax.fori_loop(0, LEVELS, level, 0)
        ends = split_dot(stacked([edge[r, p] for r in range(LEVELS + 1) for p in range(PAIRS)] ), ones[...])
        for r in range(LEVELS + 1):
            for p in range(PAIRS):
                at = (r * PAIRS + p) * 8
                corner[r, p] = corner[r, p] + ends[at : at + 8]

    prepare(lambda n: y_ref[n])
    chain()

    def tick(t, carry):
        send_note(t)
        settle(t)
        y_copy(y_ref, t, 0, next1).wait_recv()

        @pl.when(t + 2 < HOPS)
        def _():
            y_copy(ybuf.at[t], t + 2, t + 2, next2).start()

        prepare(lambda n: ybuf[t, n])
        note_copy(t).wait_recv()
        got = heard[t]
        for p in range(PAIRS):
            rise = jnp.broadcast_to(got[p : p + 1], (8, TILE))
            from_corner = jnp.broadcast_to(got[PAIRS + p : PAIRS + p + 1], (8, TILE))
            rise = rise + jnp.where(lane_row == 0, from_corner - corner[0, p], 0.0)
            edge[0, p] = jnp.where(at_start, 0.0, rise)
        chain()
        return carry

    lax.fori_loop(0, HOPS, tick, 0)
    settle(HOPS)
    for r in range(LEVELS):
        found = []
        for p in range(PAIRS):
            row = all_rows(jnp.where(row_here == lane + 1, lam[r, p], 0.0)) + corner[r, p]
            found.append(jnp.where(lane_row == TILE - 1, corner[r + 1, p], row))
        right_ref[:, r * TILE : (r + 1) * TILE] = rows_of_pairs(found)[:PAIRS]

    x_copy().wait_send()
    for s in range(HOPS):
        y_copy(y_ref, s, s, next1).wait_send()
        note_copy(s).wait_send()


def local(x_path, x_anchor, y_steps, left_in, bottom_in, corner_in):
    tile = (LEVELS, PAIRS, TILE, TILE)
    row = (LEVELS + 1, PAIRS, 8, TILE)
    vmem = pl.BlockSpec(memory_space=pltpu.VMEM)
    dma = pltpu.SemaphoreType.DMA
    return pl.pallas_call(
        kernel,
        out_shape=(
            jax.ShapeDtypeStruct((PAIRS, LEVELS * TILE), F32),
            jax.ShapeDtypeStruct((PAIRS, TICKS * TILE), F32),
        ),
        in_specs=[vmem] * 6,
        out_specs=(vmem, vmem),
        scratch_shapes=[
            pltpu.VMEM(x_path.shape, BF16),
            *[pltpu.VMEM(tile, F32) for _ in range(6)],
            pltpu.VMEM(row, F32),
            pltpu.VMEM(row, F32),
            pltpu.VMEM((2 * TILE, TILE), BF16),
            pltpu.VMEM((2 * TILE, TILE), BF16),
            pltpu.VMEM((8, TILE), F32),
            pltpu.VMEM((8, TILE), F32),
            pltpu.VMEM((HOPS, *y_steps.shape), BF16),
            pltpu.VMEM((HOPS, 8, TILE), F32),
            pltpu.VMEM((HOPS, 8, TILE), F32),
            dma, dma, dma((HOPS,)), dma((HOPS,)), dma((HOPS,)), dma((HOPS,)),
        ],
        compiler_params=pltpu.CompilerParams(collective_id=0, has_side_effects=True, vmem_limit_bytes=40 * 1024 * 1024),
        name="goursat",
    )(x_path, x_anchor, y_steps, left_in, bottom_in, corner_in)


def solution(mesh):
    placed = (
        P("pair", "tm", None),
        P("pair", None),
        P("pair", "tm", None),
        P("pair", "tm"),
        P("pair", "tm"),
        P("pair", "tm"),
    )
    return jax.shard_map(
        local,
        mesh=mesh,
        in_specs=placed,
        out_specs=(P("pair", "tm"), P("pair", "tm")),
        check_vma=False,
    )
```

```python
import functools

import jax
import jax.numpy as jnp
from jax import lax
from jax.experimental import pallas as pl
from jax.experimental.pallas import tpu as pltpu
from jax.sharding import PartitionSpec as P

MESH = pl.DeviceIdType.MESH
TICKS = 6
HOPS = TICKS - 1
TILE = 128
LEVELS = 4
PAIRS = 4
GROUPS = TILE // 8
F32 = jnp.float32
BF16 = jnp.bfloat16


def iota(shape, axis):
    return lax.broadcasted_iota(jnp.int32, shape, axis)


def tile_row(shape):
    place = iota(shape, 0)
    return (place % 8) * GROUPS + place // 8


def split_dot(rows, weights):
    high = rows.astype(BF16)
    low = (rows - high.astype(F32)).astype(BF16)
    return jnp.dot(jnp.concatenate([high, low], axis=1), weights, preferred_element_type=F32)


def vectors(tile):
    return [tile[8 * j : 8 * j + 8] for j in range(GROUPS)]


def stacked(parts):
    return jnp.concatenate(parts, axis=0)


def before_rows(tile, start=None):
    sub = iota((8, TILE), 0)
    running = jnp.zeros((8, TILE), F32)
    sums = []
    for part in vectors(tile):
        sums.append(running)
        running = running + part
    scan = running
    for step in (1, 2, 4):
        scan = scan + jnp.where(sub >= step, pltpu.roll(scan, step, axis=0), 0.0)
    offset = scan - running if start is None else scan - running + start
    return stacked([s + offset for s in sums])


def all_rows(tile):
    parts = vectors(tile)
    while len(parts) > 1:
        parts = [a + b for a, b in zip(parts[::2], parts[1::2])]
    total = parts[0]
    for step in (4, 2, 1):
        total = total + pltpu.roll(total, step, axis=0)
    return total


def repeated(row):
    return stacked([row] * GROUPS)


def rows_of_pairs(values):
    sub = iota((8, TILE), 0)
    out = values[-1]
    for k in range(len(values) - 2, -1, -1):
        out = jnp.where(sub == k, values[k], out)
    return out


def kernel(
    x_hbm, anchor_hbm, y_hbm, left_hbm, bottom_hbm, corner_hbm, right_ref, top_ref,
    x_ref, tail_ref, anchor_ref, y_ref, left_ref, bottom_ref, corner_ref, load,
    steps, prod, minus, plus, lead, base, lam, last, edge, corner, tri, ones,
    xs, xgot, ybuf, note, heard,
    xs_send, xs_recv, y_send, y_recv, note_send, note_recv,
):
    count = lax.axis_size("tm")
    me, part = lax.axis_index("tm"), lax.axis_index("pair")
    at_start = me == 0
    next1, next2 = lax.rem(me + 1, count), lax.rem(me + 2, count)
    prev1, prev2 = lax.rem(me + count - 1, count), lax.rem(me + count - 2, count)

    barrier = pltpu.get_barrier_semaphore()
    for other in (prev1, prev2):
        pl.semaphore_signal(barrier, inc=1, device_id=(other, part), device_id_type=MESH)

    loads = [
        pltpu.make_async_copy(source, target, load.at[k])
        for k, (source, target) in enumerate((
            (x_hbm.at[:, LEVELS * TILE - 16 : LEVELS * TILE, :], tail_ref),
            (y_hbm, y_ref),
            (left_hbm, left_ref),
            (bottom_hbm, bottom_ref),
            (corner_hbm, corner_ref),
            (x_hbm, x_ref),
            (anchor_hbm, anchor_ref),
        ))
    ]
    for copy in loads:
        copy.start()

    def x_copy():
        return pltpu.make_async_remote_copy(
            src_ref=xs, dst_ref=xgot, send_sem=xs_send, recv_sem=xs_recv,
            device_id=(next1, part), device_id_type=MESH,
        )

    def y_copy(source, slot, sem, to):
        return pltpu.make_async_remote_copy(
            src_ref=source, dst_ref=ybuf.at[slot], send_sem=y_send.at[sem], recv_sem=y_recv.at[slot],
            device_id=(to, part), device_id_type=MESH,
        )

    def note_copy(t):
        return pltpu.make_async_remote_copy(
            src_ref=note.at[t], dst_ref=heard.at[t], send_sem=note_send.at[t], recv_sem=note_recv.at[t],
            device_id=(next1, part), device_id_type=MESH,
        )

    loads[0].wait()
    for m in range(2):
        tail = tail_ref[m].astype(F32)[15:16]
        for c in range(4):
            xs[m * 4 + c : m * 4 + c + 1, :] = tail[:, c * 128 : (c + 1) * 128]
    loads[1].wait()

    pl.semaphore_wait(barrier, 2)

    @pl.when(me < count - 1)
    def _():
        x_copy().start()

    y_copy(y_ref, 0, 0, next1).start()

    from_row = iota((2 * TILE, TILE), 0) % TILE
    tri[...] = jnp.where(from_row < iota((2 * TILE, TILE), 1), 1.0, 0.0).astype(BF16)
    ones[...] = jnp.ones((2 * TILE, TILE), BF16)
    row_here, lane = tile_row((TILE, TILE)), iota((TILE, TILE), 1)
    differ = jnp.where(lane == row_here, 1.0, jnp.where(lane == row_here - 1, -1.0, 0.0)).astype(BF16)
    lane_row = iota((8, TILE), 1)

    for copy in loads[2:]:
        copy.wait()
    for p in range(PAIRS):
        start = jnp.broadcast_to(corner_ref[0:1, p : p + 1], (8, TILE))
        start = jnp.where(at_start, 1.0, start)
        corner[0, p] = start
        for r in range(LEVELS):
            at = (r + 1) * TILE - 1
            corner[r + 1, p] = jnp.broadcast_to(left_ref[p : p + 1, at : at + 1], (8, TILE))
        bottom = jnp.broadcast_to(bottom_ref[p : p + 1, :], (8, TILE))
        shifted = jnp.where(lane_row == 0, start, pltpu.roll(bottom, 1, axis=1))
        edge[0, p] = jnp.where(at_start, 0.0, bottom - shifted)
    for r in range(LEVELS):
        picked = []
        for p in range(PAIRS):
            row = jnp.broadcast_to(left_ref[p : p + 1, r * TILE : (r + 1) * TILE], (8, TILE)) - corner[r, p]
            picked.append(jnp.where(lane == row_here - 1, repeated(row), 0.0))
        spread = split_dot(stacked(picked), ones[...])
        for p in range(PAIRS):
            lam[r, p] = spread[p * TILE : (p + 1) * TILE]

    def increments(m, r, previous):
        found = jnp.dot(differ, x_ref[m, r * TILE : (r + 1) * TILE, :], preferred_element_type=F32)
        found = jnp.where(iota((TILE, 512), 0) == 0, found - previous, found)
        steps[m, r * TILE : (r + 1) * TILE, :] = found.astype(BF16)

    def products(y_of, first, last_level):
        for m in range(2):
            for n in range(2):
                found = lax.dot_general(
                    steps[m, first * TILE : last_level * TILE, :], y_of(n), (((1,), (1,)), ((), ())),
                    preferred_element_type=F32,
                )
                for r in range(first, last_level):
                    prod[r, 2 * m + n] = found[(r - first) * TILE : (r - first + 1) * TILE]

    def sums(r):
        for p in range(PAIRS):
            wide = split_dot(prod[r, p], tri[...])
            both = before_rows(wide)
            down = before_rows(prod[r, p])
            minus[r, p] = -(both + down)
            plus[r, p] = 1.0 + both
            edge_part = lam[r, p]
            lead[r, p] = edge_part + before_rows(edge_part * wide)
            base[r, p] = edge_part + repeated(corner[r, p])

    def chain():
        def level(r):
            bottoms = [edge[r, p] for p in range(PAIRS)]
            rows = [repeated(bottoms[p]) * minus[r, p] for p in range(PAIRS)]
            grids = [None] * PAIRS
            for p in range(PAIRS):
                out = split_dot(stacked([rows[p], bottoms[p]]), tri[...])
                low = repeated(corner[r, p] + out[TILE : TILE + 8])
                grids[p] = lead[r, p] + low * plus[r, p] + out[:TILE]
            for sweep in range(2):
                for p in range(PAIRS):
                    inside = before_rows(prod[r, p] * grids[p], bottoms[p])
                    grids[p] = base[r, p] + split_dot(inside, tri[...])
            for p in range(PAIRS):
                final = prod[r, p] * grids[p]
                last[r, p] = final
                edge[r + 1, p] = bottoms[p] + all_rows(final)

        for r in range(LEVELS):
            level(r)

    def send_note(t):
        note[t] = rows_of_pairs([edge[LEVELS, p] for p in range(PAIRS)] + [corner[LEVELS, p] for p in range(PAIRS)])

        @pl.when(me < count - 1)
        def _():
            note_copy(t).start()

    def settle(t):
        tops = [edge[LEVELS, p] for p in range(PAIRS)]
        out = split_dot(stacked(tops), tri[...])
        whole = rows_of_pairs([corner[LEVELS, p] + tops[p] + out[8 * p : 8 * p + 8] for p in range(PAIRS)])
        top_ref[:, pl.ds(pl.multiple_of(t * TILE, TILE), TILE)] = whole[:PAIRS]

        def level(r):
            for p in range(PAIRS):
                lam[r, p] = lam[r, p] + split_dot(before_rows(last[r, p]), ones[...])

        for r in range(LEVELS):
            level(r)
        ends = split_dot(stacked([edge[r, p] for r in range(LEVELS + 1) for p in range(PAIRS)] ), ones[...])
        for r in range(LEVELS + 1):
            for p in range(PAIRS):
                at = (r * PAIRS + p) * 8
                corner[r, p] = corner[r, p] + ends[at : at + 8]

    for m in range(2):
        for r in range(1, LEVELS):
            increments(m, r, x_ref[m, r * TILE - 16 : r * TILE, :].astype(F32)[15:16])
    products(lambda n: y_ref[n], 1, LEVELS)
    for r in range(1, LEVELS):
        sums(r)
    y_copy(y_ref, 1, 1, next2).start()

    @pl.when(me > 0)
    def _():
        x_copy().wait_recv()

    for m in range(2):
        came = jnp.concatenate([xgot[m * 4 + c : m * 4 + c + 1, :] for c in range(4)], axis=1)
        increments(m, 0, jnp.where(at_start, anchor_ref[m : m + 1, :].astype(F32), came))
    products(lambda n: y_ref[n], 0, 1)
    sums(0)
    chain()

    def tick(t, carry):
        send_note(t)
        settle(t)
        y_copy(y_ref, t, 0, next1).wait_recv()

        @pl.when(t + 2 < HOPS)
        def _():
            y_copy(ybuf.at[t], t + 2, t + 2, next2).start()

        products(lambda n: ybuf[t, n], 0, LEVELS)
        for r in range(LEVELS):
            sums(r)

        @pl.when(me > 0)
        def _():
            note_copy(t).wait_recv()

        got = heard[t]
        for p in range(PAIRS):
            rise = jnp.broadcast_to(got[p : p + 1], (8, TILE))
            from_corner = jnp.broadcast_to(got[PAIRS + p : PAIRS + p + 1], (8, TILE))
            rise = rise + jnp.where(lane_row == 0, from_corner - corner[0, p], 0.0)
            edge[0, p] = jnp.where(at_start, 0.0, rise)
        chain()
        return carry

    lax.fori_loop(0, HOPS, tick, 0)
    settle(HOPS)
    for r in range(LEVELS):
        found = []
        for p in range(PAIRS):
            row = all_rows(jnp.where(row_here == lane + 1, lam[r, p], 0.0)) + corner[r, p]
            found.append(jnp.where(lane_row == TILE - 1, corner[r + 1, p], row))
        right_ref[:, r * TILE : (r + 1) * TILE] = rows_of_pairs(found)[:PAIRS]

    @pl.when(me < count - 1)
    def _():
        x_copy().wait_send()
        for s in range(HOPS):
            note_copy(s).wait_send()

    for s in range(HOPS):
        y_copy(y_ref, s, s, next1).wait_send()


def local(x_path, x_anchor, y_steps, left_in, bottom_in, corner_in):
    tile = (LEVELS, PAIRS, TILE, TILE)
    row = (LEVELS + 1, PAIRS, 8, TILE)
    vmem = pl.BlockSpec(memory_space=pltpu.VMEM)
    hbm = pl.BlockSpec(memory_space=pltpu.HBM)
    dma = pltpu.SemaphoreType.DMA
    return pl.pallas_call(
        kernel,
        out_shape=(
            jax.ShapeDtypeStruct((PAIRS, LEVELS * TILE), F32),
            jax.ShapeDtypeStruct((PAIRS, TICKS * TILE), F32),
        ),
        in_specs=[hbm] * 6,
        out_specs=(vmem, vmem),
        scratch_shapes=[
            pltpu.VMEM(x_path.shape, BF16),
            pltpu.VMEM((2, 16, x_path.shape[2]), BF16),
            pltpu.VMEM(x_anchor.shape, BF16),
            pltpu.VMEM(y_steps.shape, BF16),
            pltpu.VMEM(left_in.shape, F32),
            pltpu.VMEM(bottom_in.shape, F32),
            pltpu.VMEM((1, PAIRS), F32),
            dma((7,)),
            pltpu.VMEM(x_path.shape, BF16),
            *[pltpu.VMEM(tile, F32) for _ in range(7)],
            pltpu.VMEM(row, F32),
            pltpu.VMEM(row, F32),
            pltpu.VMEM((2 * TILE, TILE), BF16),
            pltpu.VMEM((2 * TILE, TILE), BF16),
            pltpu.VMEM((8, TILE), F32),
            pltpu.VMEM((8, TILE), F32),
            pltpu.VMEM((HOPS, *y_steps.shape), BF16),
            pltpu.VMEM((HOPS, 8, TILE), F32),
            pltpu.VMEM((HOPS, 8, TILE), F32),
            dma, dma, dma((HOPS,)), dma((HOPS,)), dma((HOPS,)), dma((HOPS,)),
        ],
        compiler_params=pltpu.CompilerParams(collective_id=0, has_side_effects=True, vmem_limit_bytes=67043328),
        name="goursat",
    )(x_path, x_anchor, y_steps, left_in, bottom_in, corner_in.T)


def solution(mesh):
    placed = (
        P("pair", "tm", None),
        P("pair", None),
        P("pair", "tm", None),
        P("pair", "tm"),
        P("pair", "tm"),
        P("pair", "tm"),
    )
    return jax.shard_map(
        local,
        mesh=mesh,
        in_specs=placed,
        out_specs=(P("pair", "tm"), P("pair", "tm")),
        check_vma=False,
    )
```

```python
import functools

import jax
import jax.numpy as jnp
from jax import lax
from jax.experimental import pallas as pl
from jax.experimental.pallas import tpu as pltpu
from jax.sharding import PartitionSpec as P

MESH = pl.DeviceIdType.MESH
TICKS = 6
HOPS = TICKS - 1
TILE = 128
LEVELS = 4
PAIRS = 4
GROUPS = TILE // 8
F32 = jnp.float32
BF16 = jnp.bfloat16


def iota(shape, axis):
    return lax.broadcasted_iota(jnp.int32, shape, axis)


def tile_row(shape):
    place = iota(shape, 0)
    return (place % 8) * GROUPS + place // 8


def split_dot(rows, weights):
    high = rows.astype(BF16)
    low = (rows - high.astype(F32)).astype(BF16)
    return jnp.dot(jnp.concatenate([high, low], axis=1), weights, preferred_element_type=F32)


def vectors(tile):
    return [tile[8 * j : 8 * j + 8] for j in range(GROUPS)]


def stacked(parts):
    return jnp.concatenate(parts, axis=0)


def before_rows(tile, start=None):
    sub = iota((8, TILE), 0)
    running = jnp.zeros((8, TILE), F32)
    sums = []
    for part in vectors(tile):
        sums.append(running)
        running = running + part
    scan = running
    for step in (1, 2, 4):
        scan = scan + jnp.where(sub >= step, pltpu.roll(scan, step, axis=0), 0.0)
    offset = scan - running if start is None else scan - running + start
    return stacked([s + offset for s in sums])


def all_rows(tile):
    parts = vectors(tile)
    while len(parts) > 1:
        parts = [a + b for a, b in zip(parts[::2], parts[1::2])]
    total = parts[0]
    for step in (4, 2, 1):
        total = total + pltpu.roll(total, step, axis=0)
    return total


def repeated(row):
    return stacked([row] * GROUPS)


def rows_of_pairs(values):
    sub = iota((8, TILE), 0)
    out = values[-1]
    for k in range(len(values) - 2, -1, -1):
        out = jnp.where(sub == k, values[k], out)
    return out


def kernel(
    x_hbm, anchor_hbm, y_hbm, left_hbm, bottom_hbm, corner_hbm, right_ref, top_ref,
    x_ref, tail_ref, anchor_ref, y_ref, left_ref, bottom_ref, corner_ref, load,
    steps, prod, minus, plus, lead, base, lam, last, edge, corner, tri, ones,
    xs, xgot, ybuf, note, heard,
    xs_send, xs_recv, y_send, y_recv, note_send, note_recv,
):
    count = lax.axis_size("tm")
    me, part = lax.axis_index("tm"), lax.axis_index("pair")
    at_start = me == 0
    next1, next2 = lax.rem(me + 1, count), lax.rem(me + 2, count)
    prev1, prev2 = lax.rem(me + count - 1, count), lax.rem(me + count - 2, count)

    barrier = pltpu.get_barrier_semaphore()
    for other in (prev1, prev2):
        pl.semaphore_signal(barrier, inc=1, device_id=(other, part), device_id_type=MESH)

    loads = [
        pltpu.make_async_copy(source, target, load.at[k])
        for k, (source, target) in enumerate((
            (x_hbm.at[:, LEVELS * TILE - 16 : LEVELS * TILE, :], tail_ref),
            (y_hbm, y_ref),
            (left_hbm, left_ref),
            (bottom_hbm, bottom_ref),
            (corner_hbm, corner_ref),
            (x_hbm, x_ref),
            (anchor_hbm, anchor_ref),
        ))
    ]
    for copy in loads:
        copy.start()

    def x_copy():
        return pltpu.make_async_remote_copy(
            src_ref=xs, dst_ref=xgot, send_sem=xs_send, recv_sem=xs_recv,
            device_id=(next1, part), device_id_type=MESH,
        )

    def y_copy(source, slot, sem, to):
        return pltpu.make_async_remote_copy(
            src_ref=source, dst_ref=ybuf.at[slot], send_sem=y_send.at[sem], recv_sem=y_recv.at[slot],
            device_id=(to, part), device_id_type=MESH,
        )

    def note_copy(t):
        return pltpu.make_async_remote_copy(
            src_ref=note.at[t], dst_ref=heard.at[t], send_sem=note_send.at[t], recv_sem=note_recv.at[t],
            device_id=(next1, part), device_id_type=MESH,
        )

    loads[0].wait()
    for m in range(2):
        tail = tail_ref[m].astype(F32)[15:16]
        for c in range(4):
            xs[m * 4 + c : m * 4 + c + 1, :] = tail[:, c * 128 : (c + 1) * 128]
    loads[1].wait()

    pl.semaphore_wait(barrier, 2)

    @pl.when(me < count - 1)
    def _():
        x_copy().start()

    y_copy(y_ref, 0, 0, next1).start()

    from_row = iota((2 * TILE, TILE), 0) % TILE
    tri[...] = jnp.where(from_row < iota((2 * TILE, TILE), 1), 1.0, 0.0).astype(BF16)
    ones[...] = jnp.ones((2 * TILE, TILE), BF16)
    row_here, lane = tile_row((TILE, TILE)), iota((TILE, TILE), 1)
    differ = jnp.where(lane == row_here, 1.0, jnp.where(lane == row_here - 1, -1.0, 0.0)).astype(BF16)
    lane_row = iota((8, TILE), 1)

    for copy in loads[2:]:
        copy.wait()
    for p in range(PAIRS):
        start = jnp.broadcast_to(corner_ref[0:1, p : p + 1], (8, TILE))
        start = jnp.where(at_start, 1.0, start)
        corner[0, p] = start
        for r in range(LEVELS):
            at = (r + 1) * TILE - 1
            corner[r + 1, p] = jnp.broadcast_to(left_ref[p : p + 1, at : at + 1], (8, TILE))
        bottom = jnp.broadcast_to(bottom_ref[p : p + 1, :], (8, TILE))
        shifted = jnp.where(lane_row == 0, start, pltpu.roll(bottom, 1, axis=1))
        edge[0, p] = jnp.where(at_start, 0.0, bottom - shifted)
    for r in range(LEVELS):
        picked = []
        for p in range(PAIRS):
            row = jnp.broadcast_to(left_ref[p : p + 1, r * TILE : (r + 1) * TILE], (8, TILE)) - corner[r, p]
            picked.append(jnp.where(lane == row_here - 1, repeated(row), 0.0))
        spread = split_dot(stacked(picked), ones[...])
        for p in range(PAIRS):
            lam[r, p] = spread[p * TILE : (p + 1) * TILE]

    def increments(m, r, previous):
        found = jnp.dot(differ, x_ref[m, r * TILE : (r + 1) * TILE, :], preferred_element_type=F32)
        found = jnp.where(iota((TILE, 512), 0) == 0, found - previous, found)
        steps[m, r * TILE : (r + 1) * TILE, :] = found.astype(BF16)

    def products(y_of, first, last_level):
        for m in range(2):
            for n in range(2):
                found = lax.dot_general(
                    steps[m, first * TILE : last_level * TILE, :], y_of(n), (((1,), (1,)), ((), ())),
                    preferred_element_type=F32,
                )
                for r in range(first, last_level):
                    prod[r, 2 * m + n] = found[(r - first) * TILE : (r - first + 1) * TILE]

    def sums(r):
        for p in range(PAIRS):
            wide = split_dot(prod[r, p], tri[...])
            both = before_rows(wide)
            down = before_rows(prod[r, p])
            minus[r, p] = -(both + down)
            plus[r, p] = 1.0 + both
            edge_part = lam[r, p]
            lead[r, p] = edge_part + before_rows(edge_part * wide)
            base[r, p] = edge_part + repeated(corner[r, p])

    def chain():
        def level(r):
            bottoms = [edge[r, p] for p in range(PAIRS)]
            rows = [repeated(bottoms[p]) * minus[r, p] for p in range(PAIRS)]
            grids = [None] * PAIRS
            for p in range(PAIRS):
                out = split_dot(stacked([rows[p], bottoms[p]]), tri[...])
                low = repeated(corner[r, p] + out[TILE : TILE + 8])
                grids[p] = lead[r, p] + low * plus[r, p] + out[:TILE]
            for sweep in range(2):
                for p in range(PAIRS):
                    inside = before_rows(prod[r, p] * grids[p], bottoms[p])
                    grids[p] = base[r, p] + split_dot(inside, tri[...])
            for p in range(PAIRS):
                final = prod[r, p] * grids[p]
                last[r, p] = final
                edge[r + 1, p] = bottoms[p] + all_rows(final)

        for r in range(LEVELS):
            level(r)

    def send_note(t):
        note[t] = rows_of_pairs([edge[LEVELS, p] for p in range(PAIRS)] + [corner[LEVELS, p] for p in range(PAIRS)])

        @pl.when(me < count - 1)
        def _():
            note_copy(t).start()

    def settle(t):
        tops = [edge[LEVELS, p] for p in range(PAIRS)]
        out = split_dot(stacked(tops), tri[...])
        whole = rows_of_pairs([corner[LEVELS, p] + tops[p] + out[8 * p : 8 * p + 8] for p in range(PAIRS)])
        top_ref[:, pl.ds(pl.multiple_of(t * TILE, TILE), TILE)] = whole[:PAIRS]

        def level(r):
            for p in range(PAIRS):
                lam[r, p] = lam[r, p] + split_dot(before_rows(last[r, p]), ones[...])

        for r in range(LEVELS):
            level(r)
        ends = split_dot(stacked([edge[r, p] for r in range(LEVELS + 1) for p in range(PAIRS)] ), ones[...])
        for r in range(LEVELS + 1):
            for p in range(PAIRS):
                at = (r * PAIRS + p) * 8
                corner[r, p] = corner[r, p] + ends[at : at + 8]

    for m in range(2):
        for r in range(1, LEVELS):
            increments(m, r, x_ref[m, r * TILE - 16 : r * TILE, :].astype(F32)[15:16])
    products(lambda n: y_ref[n], 1, LEVELS)
    for r in range(1, LEVELS):
        sums(r)

    @pl.when(me < count - 2)
    def _():
        y_copy(y_ref, 1, 1, next2).start()


    @pl.when(me > 0)
    def _():
        x_copy().wait_recv()

    for m in range(2):
        came = jnp.concatenate([xgot[m * 4 + c : m * 4 + c + 1, :] for c in range(4)], axis=1)
        increments(m, 0, jnp.where(at_start, anchor_ref[m : m + 1, :].astype(F32), came))
    products(lambda n: y_ref[n], 0, 1)
    sums(0)
    chain()

    def tick(t, carry):
        def arrival():
            y_copy(y_ref, t, 0, next1).wait_recv()

        def onward():
            y_copy(ybuf.at[t], t + 2, t + 2, next2).start()

        send_note(t)

        @pl.when(t > 0)
        def _():
            pl.when(t > 0)(arrival)

            @pl.when(t + 2 < HOPS)
            def _():
                onward()

        @pl.when((t == 0) & (me >= count - 2))
        def _():
            y_copy(y_ref, 1, 1, next2).start()

        settle(t)

        @pl.when(t == 0)
        def _():
            arrival()
            onward()

        products(lambda n: ybuf[t, n], 0, LEVELS)
        for r in range(LEVELS):
            sums(r)

        @pl.when(me > 0)
        def _():
            note_copy(t).wait_recv()

        got = heard[t]
        for p in range(PAIRS):
            rise = jnp.broadcast_to(got[p : p + 1], (8, TILE))
            from_corner = jnp.broadcast_to(got[PAIRS + p : PAIRS + p + 1], (8, TILE))
            rise = rise + jnp.where(lane_row == 0, from_corner - corner[0, p], 0.0)
            edge[0, p] = jnp.where(at_start, 0.0, rise)
        chain()
        return carry

    lax.fori_loop(0, HOPS, tick, 0)
    settle(HOPS)
    for r in range(LEVELS):
        found = []
        for p in range(PAIRS):
            row = all_rows(jnp.where(row_here == lane + 1, lam[r, p], 0.0)) + corner[r, p]
            found.append(jnp.where(lane_row == TILE - 1, corner[r + 1, p], row))
        right_ref[:, r * TILE : (r + 1) * TILE] = rows_of_pairs(found)[:PAIRS]

    @pl.when(me < count - 1)
    def _():
        x_copy().wait_send()
        for s in range(HOPS):
            note_copy(s).wait_send()

    for s in range(HOPS):
        y_copy(y_ref, s, s, next1).wait_send()


def local(x_path, x_anchor, y_steps, left_in, bottom_in, corner_in):
    tile = (LEVELS, PAIRS, TILE, TILE)
    row = (LEVELS + 1, PAIRS, 8, TILE)
    vmem = pl.BlockSpec(memory_space=pltpu.VMEM)
    hbm = pl.BlockSpec(memory_space=pltpu.HBM)
    dma = pltpu.SemaphoreType.DMA
    return pl.pallas_call(
        kernel,
        out_shape=(
            jax.ShapeDtypeStruct((PAIRS, LEVELS * TILE), F32),
            jax.ShapeDtypeStruct((PAIRS, TICKS * TILE), F32),
        ),
        in_specs=[hbm] * 6,
        out_specs=(vmem, vmem),
        scratch_shapes=[
            pltpu.VMEM(x_path.shape, BF16),
            pltpu.VMEM((2, 16, x_path.shape[2]), BF16),
            pltpu.VMEM(x_anchor.shape, BF16),
            pltpu.VMEM(y_steps.shape, BF16),
            pltpu.VMEM(left_in.shape, F32),
            pltpu.VMEM(bottom_in.shape, F32),
            pltpu.VMEM((1, PAIRS), F32),
            dma((7,)),
            pltpu.VMEM(x_path.shape, BF16),
            *[pltpu.VMEM(tile, F32) for _ in range(7)],
            pltpu.VMEM(row, F32),
            pltpu.VMEM(row, F32),
            pltpu.VMEM((2 * TILE, TILE), BF16),
            pltpu.VMEM((2 * TILE, TILE), BF16),
            pltpu.VMEM((8, TILE), F32),
            pltpu.VMEM((8, TILE), F32),
            pltpu.VMEM((HOPS, *y_steps.shape), BF16),
            pltpu.VMEM((HOPS, 8, TILE), F32),
            pltpu.VMEM((HOPS, 8, TILE), F32),
            dma, dma, dma((HOPS,)), dma((HOPS,)), dma((HOPS,)), dma((HOPS,)),
        ],
        compiler_params=pltpu.CompilerParams(collective_id=0, has_side_effects=True, vmem_limit_bytes=67043328),
        name="goursat",
    )(x_path, x_anchor, y_steps, left_in, bottom_in, corner_in.T)


def solution(mesh):
    placed = (
        P("pair", "tm", None),
        P("pair", None),
        P("pair", "tm", None),
        P("pair", "tm"),
        P("pair", "tm"),
        P("pair", "tm"),
    )
    return jax.shard_map(
        local,
        mesh=mesh,
        in_specs=placed,
        out_specs=(P("pair", "tm"), P("pair", "tm")),
        check_vma=False,
    )
```
